32 devices in a mesh: grp: 2 (over y), blk: 16 (over z, x, core).
Axes of the slice: x: 2, y: 2, z: 4, core: 2. Of those that a mesh axis runs over, the one named last changes fastest.
Arguments:
- query_rows: bfloat16 [3072, 4096], P('blk', 'grp'), may hold values from -128 to 128
- key_rows: bfloat16 [3072, 512], P(('grp', 'blk')), may hold values from -6 to 6
- value_rows: bfloat16 [3072, 512], P(('grp', 'blk')), may hold values from -6 to 6
- span_ids: int32 [32], P('blk'), may hold values from 0 to 31, as said below
Outputs:
- attended: bfloat16 [3072, 4096], P('blk', 'grp')
The draws below stay inside these ranges and needn't reach their ends.
Inputs may be any that keep to these rules, and one draw needn't show every extreme that they name: `span_ids`: A permutation of 0 to 31; each device of blk holds two entries, in device order.
All inputs are finite; a program needn't handle non-finite values.
Results may differ from the reference program's by a relative error of at most 0.0045.
Values may be sent and summed in bfloat16 or wider, within the bound.
A program may use at most 64 MiB of HBM per device.

```python
import math
import jax
import jax.numpy as jnp
from jax import lax

HEADS = 32
KV_HEADS = 4
HEAD_DIM = 128
SPAN = 96
SEQ = 3072
SPANS = 32


def shared_keys(key):
    raw = jax.random.normal(jax.random.fold_in(key, 7), (SEQ, KV_HEADS, HEAD_DIM), jnp.float32)
    return jnp.clip(raw, -5.0, 5.0)


def draw_query_rows(key, part):
    base = jax.random.normal(jax.random.fold_in(key, 3), (SEQ, HEADS * HEAD_DIM), jnp.float32)
    base = 3.0 * jnp.clip(base, -6.0, 6.0)
    return base.astype(jnp.bfloat16)


def draw_key_rows(key, part):
    keys_out = shared_keys(key)
    return keys_out.reshape(SEQ, KV_HEADS * HEAD_DIM).astype(jnp.bfloat16)


def draw_span_ids(key, part):
    return jax.random.permutation(jax.random.fold_in(key, 11), SPANS).astype(jnp.int32)


def shard_levels(key, extent, cuts, least, high):
    def one(dim, parts):
        heights = jax.random.uniform(jax.random.fold_in(jax.random.fold_in(key, 6), dim), (parts,), jnp.float32, least / len(cuts), high / len(cuts))
        return jnp.repeat(jnp.exp(heights), extent[dim] // parts).reshape((-1,) + (1,) * (len(extent) - dim - 1))

    factor_of = one(*cuts[0])
    for cut in cuts[1:]:
        factor_of = factor_of * one(*cut)
    return factor_of


def normal_values(key, shape, spread, limit, pieces=(), held_as=jnp.bfloat16):
    entries = jax.random.normal(key, shape, jnp.float32) * spread
    if len(pieces) > 0:
        entries = shard_levels(key, shape, pieces, -0.22, 0.18) * entries
    return jnp.clip(entries, min=-limit, max=limit).astype(held_as)


def setup_inputs(seed: int = 0) -> dict:
    streams_of = jax.random.split(jax.random.key(seed), 5)
    query_rows = draw_query_rows(jax.random.fold_in(streams_of[4], 71), 0)
    key_rows = draw_key_rows(jax.random.fold_in(streams_of[4], 71), 0)
    value_rows = normal_values(streams_of[2], (SEQ, KV_HEADS * HEAD_DIM), 1.0, 6.0, ((0, 32),))
    span_ids = draw_span_ids(jax.random.fold_in(streams_of[4], 71), 0)
    return dict(query_rows=query_rows, key_rows=key_rows, value_rows=value_rows, span_ids=span_ids)


def reference(query_rows, key_rows, value_rows, span_ids):
    rows = jnp.arange(SEQ, dtype=jnp.int32)
    positions = (span_ids[rows // SPAN] * SPAN + rows % SPAN).astype(jnp.int32)
    ratio = HEADS // KV_HEADS
    scale = HEAD_DIM ** -0.5
    keys_all = key_rows.reshape(SEQ, KV_HEADS, HEAD_DIM).astype(jnp.float32)
    values_all = value_rows.reshape(SEQ, KV_HEADS, HEAD_DIM).astype(jnp.float32)
    block_rows = math.gcd(SEQ, 256)

    def one_block(start):
        query_block = lax.dynamic_slice_in_dim(query_rows, start, block_rows, 0)
        query_block = query_block.reshape(block_rows, KV_HEADS, ratio, HEAD_DIM).astype(jnp.float32)
        query_pos = lax.dynamic_slice_in_dim(positions, start, block_rows, 0)
        scores = jnp.einsum('tgrd,ngd->grtn', query_block, keys_all) * scale
        allowed = positions[None, :] <= query_pos[:, None]
        scores = jnp.where(allowed, scores, -jnp.inf)
        top = jnp.max(scores, axis=-1, keepdims=True)
        weights = jnp.where(allowed, jnp.exp(scores - top), 0.0).astype(jnp.bfloat16)
        weights_wide = weights.astype(jnp.float32)
        total = jnp.sum(weights_wide, axis=-1)
        mixed = jnp.einsum('grtn,ngd->grtd', weights_wide, values_all) / total[..., None]
        mixed = jnp.transpose(mixed, (2, 0, 1, 3)).reshape(block_rows, HEADS * HEAD_DIM)
        return mixed.astype(jnp.bfloat16)

    starts = (jnp.arange(SEQ // block_rows) * block_rows).astype(jnp.int32)
    blocks_out = lax.map(one_block, starts)
    return blocks_out.reshape(SEQ, HEADS * HEAD_DIM)
```

```python
import functools
import math

import jax
import jax.numpy as jnp
from jax import lax
from jax.experimental import pallas as pl
from jax.experimental.pallas import tpu as pltpu
from jax.sharding import PartitionSpec as P

MESH = pl.DeviceIdType.MESH
FAR = -1e30

HEAD_DIM = 128


def safe_top(values):
    return jnp.where(values == -jnp.inf, 0.0, values)


def attend(state, query_heads, query_pos, keys_block, values_block, key_pos):
    mark, total, weighted = state
    scale = query_heads.shape[-1] ** (-0.5)
    scores = (
        jnp.einsum("tgrd,ngd->grtn", query_heads, keys_block, preferred_element_type=jnp.float32)
        * scale
    )
    allowed = key_pos[None, :] <= query_pos[:, None]
    scores = jnp.where(allowed, scores, -jnp.inf)
    fresh = jnp.maximum(mark, jnp.max(scores, axis=-1))
    steady = safe_top(fresh)
    factor = jnp.exp(mark - steady)
    weights = jnp.where(allowed, jnp.exp(scores - steady[..., None]), 0.0).astype(jnp.bfloat16)
    total = total * factor + jnp.sum(weights.astype(jnp.float32), axis=-1)
    update = jnp.einsum("grtn,ngd->grtd", weights, values_block, preferred_element_type=jnp.float32)
    weighted = weighted * factor[..., None] + update
    return (fresh, total, weighted)


def lookup_ids(table, indices):
    columns = jnp.arange(table.shape[0], dtype=jnp.int32)
    matches = indices[:, None] == columns[None, :]
    return jnp.sum(jnp.where(matches, table[None, :], 0), axis=1)


def pick_width(count, limit):
    chosen = 1
    for trial in range(1, min(count, limit) + 1):
        if count % trial == 0:
            chosen = trial
    return chosen


def fold_keys(state_in, piece, query_heads, query_pos, table, locate, span_len, limit):
    count = piece.shape[1]
    width = pick_width(count, limit)
    steps_count = count // width
    pieces = jnp.moveaxis(piece.reshape((2, steps_count, width) + piece.shape[2:]), 1, 0)
    offsets = jnp.arange(steps_count, dtype=jnp.int32) * width

    def step(carry, item):
        pair_now, offset = item
        gathered = offset + jnp.arange(width, dtype=jnp.int32)
        stored = locate(gathered)
        key_pos = lookup_ids(table, stored // span_len) * span_len + stored % span_len
        result = attend(carry, query_heads, query_pos, pair_now[0], pair_now[1], key_pos)
        return (result, None)

    return lax.scan(step, state_in, (pieces, offsets))[0]


def empty_state(kv_count, per_kv, tokens):
    return (
        jnp.full((kv_count, per_kv, tokens), -jnp.inf, jnp.float32),
        jnp.zeros((kv_count, per_kv, tokens), jnp.float32),
        jnp.zeros((kv_count, per_kv, tokens, HEAD_DIM), jnp.float32),
    )


def fits_kernel(query_rows, key_rows):
    groups, blocks = lax.axis_size("grp"), lax.axis_size("blk")
    span_len = query_rows.shape[0] // 2
    return (
        groups == 2
        and blocks % 4 == 0
        and key_rows.shape[1] == 2 * groups * HEAD_DIM
        and key_rows.shape[0] == span_len
        and span_len % 16 == 0
        and span_len < HEAD_DIM
        and query_rows.shape[1] % (2 * HEAD_DIM) == 0
    )


def attention_kernel(
    planes, span, per_kv, rows_at_once,
    q_hbm, k_hbm, v_hbm, id_ref, out_ref,
    kv, stage, ids, qraw, qaug_q, kp, vp, onehot, acc, mark, obuf,
    load_sem, swap_send, swap_recv, id_send, id_recv, q_sem,
    up_send, down_send, x_send, z_recv, x_recv, out_sem,
):
    y = lax.axis_index("grp")
    blk = lax.axis_index("blk")
    z, x, c = blk // 4, (blk // 2) % 2, blk % 2
    blocks = 4 * planes
    wide = per_kv * HEAD_DIM
    rows = per_kv * span
    keys = 8 * span
    other_y, other_x, other_c = 1 - y, 1 - x, 1 - c
    sibling = (y, z * 4 + x * 2 + other_c)
    across = (y, z * 4 + other_x * 2 + c)

    def place(at_z):
        return (y, at_z * 4 + x * 2 + c)

    def remote(src, dst, send, recv, target):
        return pltpu.make_async_remote_copy(
            src_ref=src, dst_ref=dst, send_sem=send, recv_sem=recv,
            device_id=target, device_id_type=MESH,
        )

    def load(head, half):
        source = (k_hbm, v_hbm)[half]
        return pltpu.make_async_copy(
            source.at[:, pl.ds(head * HEAD_DIM, HEAD_DIM)],
            stage.at[head, :, pl.ds(half * HEAD_DIM, HEAD_DIM)],
            load_sem.at[head, half],
        )

    def load_own(half):
        source = (k_hbm, v_hbm)[half]
        return pltpu.make_async_copy(
            source.at[:, pl.ds(pl.multiple_of((2 * y + c) * HEAD_DIM, HEAD_DIM), HEAD_DIM)],
            kv.at[z, x, y, c, :, pl.ds(half * HEAD_DIM, HEAD_DIM)],
            load_sem.at[4, half],
        )

    for head in range(4):
        for half in range(2):
            load(head, half).start()
    for half in range(2):
        load_own(half).start()

    barrier = pltpu.get_barrier_semaphore()

    @pl.loop(1, blocks)
    def _(step):
        pl.semaphore_signal(
            barrier, inc=1, device_id=(y, lax.rem(blk + step, blocks)), device_id_type=MESH
        )

    for target_c in (c, other_c):
        pl.semaphore_signal(
            barrier, inc=1, device_id=(other_y, z * 4 + x * 2 + target_c), device_id_type=MESH
        )

    token = lax.broadcasted_iota(jnp.int32, (span, HEAD_DIM), 0)
    lane = lax.broadcasted_iota(jnp.int32, (span, HEAD_DIM), 1)
    onehot[...] = jnp.where((lane == token) | (lane == span), 1.0, 0.0).astype(jnp.bfloat16)
    penalty = jnp.where(
        ((lane > token) & (lane < span)) | (lane == span), FAR, 0.0
    ).astype(jnp.bfloat16)
    for slot in range(4):
        for r in range(per_kv):
            qaug_q[slot, r * span : (r + 1) * span, HEAD_DIM:] = penalty
    vp[:, HEAD_DIM:] = jnp.ones((keys, HEAD_DIM), jnp.bfloat16)
    mark[...] = jnp.full(mark.shape, -3e38, jnp.float32)
    acc[...] = jnp.zeros(acc.shape, jnp.float32)
    for head in range(4):
        for half in range(2):
            load(head, half).wait()
    for half in range(2):
        load_own(half).wait()
    pl.semaphore_wait(barrier, blocks + 1)

    def swap(slot):
        to_y = (y, other_y, other_y)[slot]
        to_c = (other_c, c, other_c)[slot]
        return remote(
            stage.at[2 * to_y + to_c], kv.at[z, x, y, c],
            swap_send.at[slot], swap_recv.at[slot], (to_y, z * 4 + x * 2 + to_c),
        )

    for slot in range(3):
        swap(slot).start()

    def id_copy(step):
        return remote(
            id_ref, ids.at[blk], id_send.at[step], id_recv.at[step],
            (y, lax.rem(blk + step, blocks)),
        )

    own_id = pltpu.make_async_copy(id_ref, ids.at[blk], id_send.at[0])
    own_id.start()

    @pl.loop(1, blocks)
    def _(step):
        id_copy(step).start()

    def q_columns(core):
        return pl.ds(pl.multiple_of(core * wide, HEAD_DIM), wide)

    q_away = remote(q_hbm.at[:, q_columns(other_c)], qraw.at[0], q_sem.at[0], q_sem.at[1], sibling)
    q_here = pltpu.make_async_copy(q_hbm.at[:, q_columns(c)], qraw.at[1], q_sem.at[2])
    q_away.start()
    q_here.start()

    def up(at_z, u):
        chunk = kv.at[at_z, x, u]
        return remote(chunk, chunk, up_send.at[at_z, u], z_recv.at[at_z, u], place(z + 1))

    def down(at_z, u):
        chunk = kv.at[at_z, x, u]
        return remote(chunk, chunk, down_send.at[at_z, u], z_recv.at[at_z, u], place(z - 1))

    def over(at_z, u):
        chunk = kv.at[at_z, x, u]
        return remote(chunk, chunk, x_send.at[at_z, u], x_recv.at[at_z, u], across)

    def z_arrival(at_z, u):
        chunk = kv.at[at_z, x, u]
        return remote(chunk, chunk, up_send.at[at_z, u], z_recv.at[at_z, u], across)

    def x_arrival(at_z, u):
        chunk = kv.at[at_z, other_x, u]
        return remote(chunk, chunk, x_send.at[at_z, u], x_recv.at[at_z, u], across)

    def pass_on(at_z, u, from_below, from_above):
        @pl.when(from_below & (z + 1 < planes))
        def _():
            up(at_z, u).start()

        @pl.when(from_above & (z > 0))
        def _():
            down(at_z, u).start()

        over(at_z, u).start()

    swap(0).wait_recv()
    pass_on(z, y, True, True)
    swap(1).wait_recv()
    swap(2).wait_recv()
    pass_on(z, other_y, True, True)

    def service(far, u):
        @pl.when((far < planes) & (z - far >= 0))
        def _():
            z_arrival(z - far, u).wait_recv()
            pass_on(z - far, u, True, False)

        @pl.when((far < planes) & (z + far < planes))
        def _():
            z_arrival(z + far, u).wait_recv()
            pass_on(z + far, u, False, True)

    q_away.wait_recv()
    q_here.wait()
    for slot in range(4):
        s = slot % 2
        for r in range(per_kv):
            qaug_q[slot, r * span : (r + 1) * span, :HEAD_DIM] = qraw[
                slot // 2, s * span : (s + 1) * span, r * HEAD_DIM : (r + 1) * HEAD_DIM
            ]
    own_id.wait()

    @pl.loop(1, blocks)
    def _(step):
        id_copy(step).wait_recv()

    factor = HEAD_DIM ** (-0.5) * math.log2(math.e)
    lane_row = lax.broadcasted_iota(jnp.int32, (1, HEAD_DIM), 1)
    near = jnp.minimum(z, planes - 1 - z)
    sign = jnp.where(z < planes - 1 - z, 1, -1)

    def plane_of(k):
        half = (k + 1) // 2
        inner = z + jnp.where(k % 2 == 1, -half, half)
        return jnp.where(k <= 2 * near, inner, z + sign * (k - near))

    def finish(slot):
        s = slot % 2
        for r in range(per_kv):
            both = acc[slot, r * span : (r + 1) * span, :]
            obuf[slot // 2, pl.ds(pl.multiple_of(s * span, 16), span), r * HEAD_DIM : (r + 1) * HEAD_DIM] = (
                both[:, :HEAD_DIM] / both[:, HEAD_DIM:]
            ).astype(jnp.bfloat16)

    out_away = remote(obuf.at[0], out_ref.at[:, q_columns(c)], out_sem.at[0], out_sem.at[1], sibling)
    out_here = pltpu.make_async_copy(obuf.at[1], out_ref.at[:, q_columns(c)], out_sem.at[2])

    @pl.loop(0, 4 * planes)
    def _(t):
        k, slot = t // 4, t % 4
        p = plane_of(k)

        @pl.when(slot == 0)
        def _():
            service(k + 1, y)
            x_arrival(p, y).wait_recv()
            x_arrival(p, other_y).wait_recv()
            plane = kv[p].reshape(keys, 2 * HEAD_DIM)
            kp[:, :HEAD_DIM] = plane[:, :HEAD_DIM]
            vp[:, :HEAD_DIM] = plane[:, HEAD_DIM:]

        @pl.when(slot == 2)
        def _():
            service(k + 1, other_y)

        owner = z * 4 + x * 2 + jnp.where(slot < 2, other_c, c)
        id_q = ids[owner, pl.ds(slot % 2, 1), :]
        for j in range(8):
            kx, ky, kc = j // 4, (j // 2) % 2, j % 2
            id_k = ids[ky * (blocks // 2) + p * 2 + kx, kc : kc + 1, :]
            same = jnp.where(id_k == id_q, 1.0, 0.0)
            later = jnp.where(id_k > id_q, 1.0, 0.0)
            choice = jnp.where(lane_row < span, same, later).astype(jnp.bfloat16)
            kp[j * span : (j + 1) * span, HEAD_DIM:] = onehot[...] * choice

        kmat = kp[...]
        vmat = vp[...]
        for first in range(0, rows, rows_at_once):
            part = pl.ds(first, rows_at_once)
            scores = lax.dot_general(
                qaug_q[slot, part, :], kmat, (((1,), (1,)), ((), ())),
                preferred_element_type=jnp.float32,
            )
            before = mark[slot, part, :]
            fresh = jnp.maximum(before, jnp.max(scores, axis=1, keepdims=True))
            mark[slot, part, :] = fresh
            weights = jnp.exp2((scores - fresh[:, :1]) * factor).astype(jnp.bfloat16)
            fade = jnp.exp2((before - fresh) * factor)
            update = jnp.dot(weights, vmat, preferred_element_type=jnp.float32)
            acc[slot, part, :HEAD_DIM] = acc[slot, part, :HEAD_DIM] * fade + update[:, :HEAD_DIM]
            acc[slot, part, HEAD_DIM:] = acc[slot, part, HEAD_DIM:] * fade + update[:, HEAD_DIM:]

        @pl.when(k == planes - 1)
        def _():
            finish(slot)

        @pl.when((k == planes - 1) & (slot == 2))
        def _():
            out_away.start()

    out_here.start()
    for slot in range(3):
        swap(slot).wait_send()
    q_away.wait_send()

    @pl.loop(1, blocks)
    def _(step):
        id_copy(step).wait_send()

    @pl.loop(0, planes)
    def _(at_z):
        for u in range(2):
            over(at_z, u).wait_send()

            @pl.when((at_z <= z) & (z + 1 < planes))
            def _():
                up(at_z, u).wait_send()

            @pl.when((at_z >= z) & (z > 0))
            def _():
                down(at_z, u).wait_send()

    out_away.wait()
    out_here.wait()


def fused(query_rows, key_rows, value_rows, span_ids):
    planes = lax.axis_size("blk") // 4
    tokens, columns = query_rows.shape
    span = tokens // 2
    per_kv = columns // (2 * HEAD_DIM)
    rows, keys, wide = per_kv * span, 8 * span, per_kv * HEAD_DIM
    id_block = jnp.broadcast_to(jnp.tile(span_ids, 4)[:, None], (8, HEAD_DIM))
    dma = pltpu.SemaphoreType.DMA
    anywhere = pl.BlockSpec(memory_space=pl.ANY)
    bf16, f32 = jnp.bfloat16, jnp.float32
    return pl.pallas_call(
        functools.partial(attention_kernel, planes, span, per_kv, math.gcd(rows, 256)),
        out_shape=jax.ShapeDtypeStruct((tokens, columns), bf16),
        in_specs=[anywhere] * 3 + [pl.BlockSpec(memory_space=pltpu.VMEM)],
        out_specs=anywhere,
        scratch_shapes=[
            pltpu.VMEM((planes, 2, 2, 2, span, 2 * HEAD_DIM), bf16),
            pltpu.VMEM((4, span, 2 * HEAD_DIM), bf16),
            pltpu.VMEM((4 * planes, 8, HEAD_DIM), jnp.int32),
            pltpu.VMEM((2, tokens, wide), bf16),
            pltpu.VMEM((4, rows, 2 * HEAD_DIM), bf16),
            pltpu.VMEM((keys, 2 * HEAD_DIM), bf16),
            pltpu.VMEM((keys, 2 * HEAD_DIM), bf16),
            pltpu.VMEM((span, HEAD_DIM), bf16),
            pltpu.VMEM((4, rows, 2 * HEAD_DIM), f32),
            pltpu.VMEM((4, rows, HEAD_DIM), f32),
            pltpu.VMEM((2, tokens, wide), bf16),
            dma((5, 2)),
            dma((3,)),
            dma((3,)),
            dma((4 * planes,)),
            dma((4 * planes,)),
            dma((3,)),
            dma((planes, 2)),
            dma((planes, 2)),
            dma((planes, 2)),
            dma((planes, 2)),
            dma((planes, 2)),
            dma((3,)),
        ],
        compiler_params=pltpu.CompilerParams(
            collective_id=0, has_side_effects=True, vmem_limit_bytes=48 * 1024 * 1024
        ),
    )(query_rows, key_rows, value_rows, id_block)


def body(query_rows, key_rows, value_rows, span_ids):
    tokens = query_rows.shape[0]
    if fits_kernel(query_rows, key_rows):
        return fused(query_rows, key_rows, value_rows, span_ids)
    span_len = tokens // 2
    kv_heads = key_rows.shape[1] // HEAD_DIM
    key_count = key_rows.shape[0]
    groups = lax.axis_size("grp")
    blocks = lax.axis_size("blk")
    blk_here = lax.axis_index("blk")
    table = lax.all_gather(span_ids, "blk", axis=0, tiled=True)
    own_ids = lax.dynamic_slice_in_dim(table, blk_here * 2, 2, 0)
    query_pos = (
        own_ids[:, None] * span_len + jnp.arange(span_len, dtype=jnp.int32)[None, :]
    ).reshape(-1)
    own_heads = query_rows.shape[1] // HEAD_DIM
    heads = own_heads * groups
    ratio = heads // kv_heads
    kv_own = max(1, own_heads // ratio)
    per_kv = own_heads // kv_own
    key_parts = []
    value_parts = []
    for target in range(groups):
        first = target * own_heads // ratio
        key_parts.append(key_rows[:, first * HEAD_DIM : (first + kv_own) * HEAD_DIM])
        value_parts.append(value_rows[:, first * HEAD_DIM : (first + kv_own) * HEAD_DIM])
    routed_keys, routed_values = (
        lax.all_to_all(jnp.stack(key_parts), "grp", split_axis=0, concat_axis=1, tiled=True),
        lax.all_to_all(jnp.stack(value_parts), "grp", split_axis=0, concat_axis=1, tiled=True),
    )
    paired = jnp.stack([routed_keys[0], routed_values[0]]).reshape(
        2, groups * key_count, kv_own, HEAD_DIM
    )
    query_heads = query_rows.reshape(tokens, kv_own, per_kv, HEAD_DIM)
    group_rows = groups * key_count

    def locate(gathered):
        source_blk = gathered // group_rows
        within = gathered % group_rows
        source_grp = within // key_count
        slot_row = within % key_count
        return ((source_grp * blocks + source_blk) * key_count + slot_row).astype(jnp.int32)

    state = fold_keys(
        empty_state(kv_own, per_kv, tokens),
        lax.all_gather(paired, "blk", axis=1, tiled=True),
        query_heads,
        query_pos,
        table,
        locate,
        span_len,
        512,
    )
    mark, total, weighted = state
    mixed = weighted / total[..., None]
    mixed = jnp.transpose(mixed, (2, 0, 1, 3)).reshape(tokens, own_heads * HEAD_DIM)
    return mixed.astype(jnp.bfloat16)


def solution(mesh):
    in_specs = (P("blk", "grp"), P(("grp", "blk"), None), P(("grp", "blk"), None), P("blk"))
    out_specs = P("blk", "grp")
    return jax.shard_map(body, mesh=mesh, in_specs=in_specs, out_specs=out_specs, check_vma=False)
```

```python
import functools
import math

import jax
import jax.numpy as jnp
from jax import lax
from jax.experimental import pallas as pl
from jax.experimental.pallas import tpu as pltpu
from jax.sharding import PartitionSpec as P

MESH = pl.DeviceIdType.MESH
FAR = -1e30

HEAD_DIM = 128


def safe_top(values):
    return jnp.where(values == -jnp.inf, 0.0, values)


def attend(state, query_heads, query_pos, keys_block, values_block, key_pos):
    mark, total, weighted = state
    scale = query_heads.shape[-1] ** (-0.5)
    scores = (
        jnp.einsum("tgrd,ngd->grtn", query_heads, keys_block, preferred_element_type=jnp.float32)
        * scale
    )
    allowed = key_pos[None, :] <= query_pos[:, None]
    scores = jnp.where(allowed, scores, -jnp.inf)
    fresh = jnp.maximum(mark, jnp.max(scores, axis=-1))
    steady = safe_top(fresh)
    factor = jnp.exp(mark - steady)
    weights = jnp.where(allowed, jnp.exp(scores - steady[..., None]), 0.0).astype(jnp.bfloat16)
    total = total * factor + jnp.sum(weights.astype(jnp.float32), axis=-1)
    update = jnp.einsum("grtn,ngd->grtd", weights, values_block, preferred_element_type=jnp.float32)
    weighted = weighted * factor[..., None] + update
    return (fresh, total, weighted)


def lookup_ids(table, indices):
    columns = jnp.arange(table.shape[0], dtype=jnp.int32)
    matches = indices[:, None] == columns[None, :]
    return jnp.sum(jnp.where(matches, table[None, :], 0), axis=1)


def pick_width(count, limit):
    chosen = 1
    for trial in range(1, min(count, limit) + 1):
        if count % trial == 0:
            chosen = trial
    return chosen


def fold_keys(state_in, piece, query_heads, query_pos, table, locate, span_len, limit):
    count = piece.shape[1]
    width = pick_width(count, limit)
    steps_count = count // width
    pieces = jnp.moveaxis(piece.reshape((2, steps_count, width) + piece.shape[2:]), 1, 0)
    offsets = jnp.arange(steps_count, dtype=jnp.int32) * width

    def step(carry, item):
        pair_now, offset = item
        gathered = offset + jnp.arange(width, dtype=jnp.int32)
        stored = locate(gathered)
        key_pos = lookup_ids(table, stored // span_len) * span_len + stored % span_len
        result = attend(carry, query_heads, query_pos, pair_now[0], pair_now[1], key_pos)
        return (result, None)

    return lax.scan(step, state_in, (pieces, offsets))[0]


def empty_state(kv_count, per_kv, tokens):
    return (
        jnp.full((kv_count, per_kv, tokens), -jnp.inf, jnp.float32),
        jnp.zeros((kv_count, per_kv, tokens), jnp.float32),
        jnp.zeros((kv_count, per_kv, tokens, HEAD_DIM), jnp.float32),
    )


def fits_kernel(query_rows, key_rows):
    groups, blocks = lax.axis_size("grp"), lax.axis_size("blk")
    span_len = query_rows.shape[0] // 2
    return (
        groups == 2
        and blocks % 4 == 0
        and key_rows.shape[1] == 2 * groups * HEAD_DIM
        and key_rows.shape[0] == span_len
        and span_len % 16 == 0
        and span_len < HEAD_DIM
        and query_rows.shape[1] % (2 * HEAD_DIM) == 0
    )


def attention_kernel(
    planes, span, per_kv, rows_at_once,
    q_hbm, k_hbm, v_hbm, id_in, out_ref,
    id_ref, kv, stage, ids, qraw, qaug_q, kp, vp, onehot, acc, mark, obuf,
    load_sem, swap_send, swap_recv, id_send, id_recv, q_sem,
    up_send, down_send, x_send, z_recv, x_recv, out_sem,
):
    y = lax.axis_index("grp")
    blk = lax.axis_index("blk")
    z, x, c = blk // 4, (blk // 2) % 2, blk % 2
    blocks = 4 * planes
    wide = per_kv * HEAD_DIM
    rows = per_kv * span
    keys = 8 * span
    other_y, other_x, other_c = 1 - y, 1 - x, 1 - c
    sibling = (y, z * 4 + x * 2 + other_c)
    across = (y, z * 4 + other_x * 2 + c)

    def place(at_z):
        return (y, at_z * 4 + x * 2 + c)

    def remote(src, dst, send, recv, target):
        return pltpu.make_async_remote_copy(
            src_ref=src, dst_ref=dst, send_sem=send, recv_sem=recv,
            device_id=target, device_id_type=MESH,
        )

    def load(head, half):
        source = (k_hbm, v_hbm)[half]
        return pltpu.make_async_copy(
            source.at[:, pl.ds(head * HEAD_DIM, HEAD_DIM)],
            stage.at[head, :, pl.ds(half * HEAD_DIM, HEAD_DIM)],
            load_sem.at[head, half],
        )

    def load_own(half):
        source = (k_hbm, v_hbm)[half]
        return pltpu.make_async_copy(
            source.at[:, pl.ds(pl.multiple_of((2 * y + c) * HEAD_DIM, HEAD_DIM), HEAD_DIM)],
            kv.at[z, x, y, c, :, pl.ds(half * HEAD_DIM, HEAD_DIM)],
            load_sem.at[4, half],
        )

    for head in range(4):
        for half in range(2):
            load(head, half).start()
    for half in range(2):
        load_own(half).start()

    for s in range(2):
        id_ref[s : s + 1, :] = jnp.full((1, HEAD_DIM), id_in[s], jnp.int32)

    barrier = pltpu.get_barrier_semaphore()

    @pl.loop(1, blocks)
    def _(step):
        pl.semaphore_signal(
            barrier, inc=1, device_id=(y, lax.rem(blk + step, blocks)), device_id_type=MESH
        )

    for target_c in (c, other_c):
        pl.semaphore_signal(
            barrier, inc=1, device_id=(other_y, z * 4 + x * 2 + target_c), device_id_type=MESH
        )

    token = lax.broadcasted_iota(jnp.int32, (span, HEAD_DIM), 0)
    lane = lax.broadcasted_iota(jnp.int32, (span, HEAD_DIM), 1)
    onehot[...] = jnp.where((lane == token) | (lane == span), 1.0, 0.0).astype(jnp.bfloat16)
    penalty = jnp.where(
        ((lane > token) & (lane < span)) | (lane == span), FAR, 0.0
    ).astype(jnp.bfloat16)
    for slot in range(2):
        for r in range(2 * per_kv):
            qaug_q[slot, r * span : (r + 1) * span, HEAD_DIM:] = penalty
    vp[:, HEAD_DIM:] = jnp.ones((keys, HEAD_DIM), jnp.bfloat16)
    mark[...] = jnp.full(mark.shape, -3e38, jnp.float32)
    acc[...] = jnp.zeros(acc.shape, jnp.float32)
    for head in range(4):
        for half in range(2):
            load(head, half).wait()
    for half in range(2):
        load_own(half).wait()
    pl.semaphore_wait(barrier, blocks + 1)

    def swap(slot):
        to_y = (y, other_y, other_y)[slot]
        to_c = (other_c, c, other_c)[slot]
        return remote(
            stage.at[2 * to_y + to_c], kv.at[z, x, y, c],
            swap_send.at[slot], swap_recv.at[slot], (to_y, z * 4 + x * 2 + to_c),
        )

    for slot in range(3):
        swap(slot).start()

    def id_copy(step):
        return remote(
            id_ref, ids.at[blk], id_send.at[step], id_recv.at[step],
            (y, lax.rem(blk + step, blocks)),
        )

    own_id = pltpu.make_async_copy(id_ref, ids.at[blk], id_send.at[0])
    own_id.start()

    @pl.loop(1, blocks)
    def _(step):
        id_copy(step).start()

    def q_columns(core):
        return pl.ds(pl.multiple_of(core * wide, HEAD_DIM), wide)

    q_away = remote(q_hbm.at[:, q_columns(other_c)], qraw.at[0], q_sem.at[0], q_sem.at[1], sibling)
    q_here = pltpu.make_async_copy(q_hbm.at[:, q_columns(c)], qraw.at[1], q_sem.at[2])
    q_away.start()
    q_here.start()

    def up(at_z, u):
        chunk = kv.at[at_z, x, u]
        return remote(chunk, chunk, up_send.at[at_z, u], z_recv.at[at_z, u], place(z + 1))

    def down(at_z, u):
        chunk = kv.at[at_z, x, u]
        return remote(chunk, chunk, down_send.at[at_z, u], z_recv.at[at_z, u], place(z - 1))

    def over(at_z, u):
        chunk = kv.at[at_z, x, u]
        return remote(chunk, chunk, x_send.at[at_z, u], x_recv.at[at_z, u], across)

    def z_arrival(at_z, u):
        chunk = kv.at[at_z, x, u]
        return remote(chunk, chunk, up_send.at[at_z, u], z_recv.at[at_z, u], across)

    def x_arrival(at_z, u):
        chunk = kv.at[at_z, other_x, u]
        return remote(chunk, chunk, x_send.at[at_z, u], x_recv.at[at_z, u], across)

    def pass_on(at_z, u, from_below, from_above):
        @pl.when(from_below & (z + 1 < planes))
        def _():
            up(at_z, u).start()

        @pl.when(from_above & (z > 0))
        def _():
            down(at_z, u).start()

        over(at_z, u).start()

    swap(0).wait_recv()
    pass_on(z, y, True, True)
    swap(1).wait_recv()
    swap(2).wait_recv()
    pass_on(z, other_y, True, True)

    def service(far, u):
        @pl.when((far < planes) & (z - far >= 0))
        def _():
            z_arrival(z - far, u).wait_recv()
            pass_on(z - far, u, True, False)

        @pl.when((far < planes) & (z + far < planes))
        def _():
            z_arrival(z + far, u).wait_recv()
            pass_on(z + far, u, False, True)

    q_away.wait_recv()
    q_here.wait()
    for slot in range(4):
        s = slot % 2
        for r in range(per_kv):
            at = (s * per_kv + r) * span
            qaug_q[slot // 2, at : at + span, :HEAD_DIM] = qraw[
                slot // 2, s * span : (s + 1) * span, r * HEAD_DIM : (r + 1) * HEAD_DIM
            ]
    own_id.wait()

    @pl.loop(1, blocks)
    def _(step):
        id_copy(step).wait_recv()

    factor = HEAD_DIM ** (-0.5) * math.log2(math.e)
    lane_row = lax.broadcasted_iota(jnp.int32, (1, HEAD_DIM), 1)
    near = jnp.minimum(z, planes - 1 - z)
    sign = jnp.where(z < planes - 1 - z, 1, -1)

    def plane_of(k):
        half = (k + 1) // 2
        inner = z + jnp.where(k % 2 == 1, -half, half)
        return jnp.where(k <= 2 * near, inner, z + sign * (k - near))

    def finish(half):
        for s in range(2):
            for r in range(per_kv):
                both = acc[half, (s * per_kv + r) * span : (s * per_kv + r + 1) * span, :]
                obuf[half, s * span : (s + 1) * span, r * HEAD_DIM : (r + 1) * HEAD_DIM] = (
                    both[:, :HEAD_DIM] / both[:, HEAD_DIM:]
                ).astype(jnp.bfloat16)

    out_away = remote(obuf.at[0], out_ref.at[:, q_columns(c)], out_sem.at[0], out_sem.at[1], sibling)
    out_here = pltpu.make_async_copy(obuf.at[1], out_ref.at[:, q_columns(c)], out_sem.at[2])

    @pl.loop(0, 2 * planes)
    def _(t):
        k, half = t // 2, t % 2
        p = plane_of(k)

        @pl.when(half == 0)
        def _():
            service(k + 1, y)
            x_arrival(p, y).wait_recv()
            x_arrival(p, other_y).wait_recv()
            plane = kv[p].reshape(keys, 2 * HEAD_DIM)
            kp[0, :, :HEAD_DIM] = plane[:, :HEAD_DIM]
            kp[1, :, :HEAD_DIM] = plane[:, :HEAD_DIM]
            vp[:, :HEAD_DIM] = plane[:, HEAD_DIM:]

        @pl.when(half == 1)
        def _():
            service(k + 1, other_y)

        owner = z * 4 + x * 2 + jnp.where(half == 0, other_c, c)
        for s in range(2):
            id_q = ids[owner, s : s + 1, :]
            for j in range(8):
                kx, ky, kc = j // 4, (j // 2) % 2, j % 2
                id_k = ids[ky * (blocks // 2) + p * 2 + kx, kc : kc + 1, :]
                same = jnp.where(id_k == id_q, 1.0, 0.0)
                later = jnp.where(id_k > id_q, 1.0, 0.0)
                choice = jnp.where(lane_row < span, same, later).astype(jnp.bfloat16)
                kp[s, j * span : (j + 1) * span, HEAD_DIM:] = onehot[...] * choice

        kmats = (kp[0], kp[1])
        vmat = vp[...]

        def score(first):
            return lax.dot_general(
                qaug_q[half, pl.ds(first, rows_at_once), :], kmats[first // rows],
                (((1,), (1,)), ((), ())), preferred_element_type=jnp.float32,
            )

        ahead = score(0)
        for first in range(0, 2 * rows, rows_at_once):
            part = pl.ds(first, rows_at_once)
            scores = ahead
            if first + rows_at_once < 2 * rows:
                ahead = score(first + rows_at_once)
            before = mark[half, part, :]
            fresh = jnp.maximum(before, jnp.max(scores, axis=1, keepdims=True))
            mark[half, part, :] = fresh
            weights = jnp.exp2((scores - fresh[:, :1]) * factor).astype(jnp.bfloat16)
            fade = jnp.exp2((before - fresh) * factor)
            update = jnp.dot(weights, vmat, preferred_element_type=jnp.float32)
            acc[half, part, :HEAD_DIM] = acc[half, part, :HEAD_DIM] * fade + update[:, :HEAD_DIM]
            acc[half, part, HEAD_DIM:] = acc[half, part, HEAD_DIM:] * fade + update[:, HEAD_DIM:]

        @pl.when(k == planes - 1)
        def _():
            finish(half)

        @pl.when((k == planes - 1) & (half == 0))
        def _():
            out_away.start()

    out_here.start()
    for slot in range(3):
        swap(slot).wait_send()
    q_away.wait_send()

    @pl.loop(1, blocks)
    def _(step):
        id_copy(step).wait_send()

    @pl.loop(0, planes)
    def _(at_z):
        for u in range(2):
            over(at_z, u).wait_send()

            @pl.when((at_z <= z) & (z + 1 < planes))
            def _():
                up(at_z, u).wait_send()

            @pl.when((at_z >= z) & (z > 0))
            def _():
                down(at_z, u).wait_send()

    out_away.wait()
    out_here.wait()


def fused(query_rows, key_rows, value_rows, span_ids):
    planes = lax.axis_size("blk") // 4
    tokens, columns = query_rows.shape
    span = tokens // 2
    per_kv = columns // (2 * HEAD_DIM)
    rows, keys, wide = per_kv * span, 8 * span, per_kv * HEAD_DIM
    dma = pltpu.SemaphoreType.DMA
    hbm = pl.BlockSpec(memory_space=pltpu.HBM)
    bf16, f32 = jnp.bfloat16, jnp.float32
    return pl.pallas_call(
        functools.partial(attention_kernel, planes, span, per_kv, math.gcd(rows, 256)),
        out_shape=jax.ShapeDtypeStruct((tokens, columns), bf16),
        in_specs=[hbm] * 3 + [pl.BlockSpec(memory_space=pltpu.SMEM)],
        out_specs=pl.BlockSpec(memory_space=pl.ANY),
        scratch_shapes=[
            pltpu.VMEM((8, HEAD_DIM), jnp.int32),
            pltpu.VMEM((planes, 2, 2, 2, span, 2 * HEAD_DIM), bf16),
            pltpu.VMEM((4, span, 2 * HEAD_DIM), bf16),
            pltpu.VMEM((4 * planes, 8, HEAD_DIM), jnp.int32),
            pltpu.VMEM((2, tokens, wide), bf16),
            pltpu.VMEM((2, 2 * rows, 2 * HEAD_DIM), bf16),
            pltpu.VMEM((2, keys, 2 * HEAD_DIM), bf16),
            pltpu.VMEM((keys, 2 * HEAD_DIM), bf16),
            pltpu.VMEM((span, HEAD_DIM), bf16),
            pltpu.VMEM((2, 2 * rows, 2 * HEAD_DIM), f32),
            pltpu.VMEM((2, 2 * rows, HEAD_DIM), f32),
            pltpu.VMEM((2, tokens, wide), bf16),
            dma((5, 2)),
            dma((3,)),
            dma((3,)),
            dma((4 * planes,)),
            dma((4 * planes,)),
            dma((3,)),
            dma((planes, 2)),
            dma((planes, 2)),
            dma((planes, 2)),
            dma((planes, 2)),
            dma((planes, 2)),
            dma((3,)),
        ],
        compiler_params=pltpu.CompilerParams(
            collective_id=0, has_side_effects=True, vmem_limit_bytes=67_000_000
        ),
    )(query_rows, key_rows, value_rows, span_ids)


def body(query_rows, key_rows, value_rows, span_ids):
    tokens = query_rows.shape[0]
    if fits_kernel(query_rows, key_rows):
        return fused(query_rows, key_rows, value_rows, span_ids)
    span_len = tokens // 2
    kv_heads = key_rows.shape[1] // HEAD_DIM
    key_count = key_rows.shape[0]
    groups = lax.axis_size("grp")
    blocks = lax.axis_size("blk")
    blk_here = lax.axis_index("blk")
    table = lax.all_gather(span_ids, "blk", axis=0, tiled=True)
    own_ids = lax.dynamic_slice_in_dim(table, blk_here * 2, 2, 0)
    query_pos = (
        own_ids[:, None] * span_len + jnp.arange(span_len, dtype=jnp.int32)[None, :]
    ).reshape(-1)
    own_heads = query_rows.shape[1] // HEAD_DIM
    heads = own_heads * groups
    ratio = heads // kv_heads
    kv_own = max(1, own_heads // ratio)
    per_kv = own_heads // kv_own
    key_parts = []
    value_parts = []
    for target in range(groups):
        first = target * own_heads // ratio
        key_parts.append(key_rows[:, first * HEAD_DIM : (first + kv_own) * HEAD_DIM])
        value_parts.append(value_rows[:, first * HEAD_DIM : (first + kv_own) * HEAD_DIM])
    routed_keys, routed_values = (
        lax.all_to_all(jnp.stack(key_parts), "grp", split_axis=0, concat_axis=1, tiled=True),
        lax.all_to_all(jnp.stack(value_parts), "grp", split_axis=0, concat_axis=1, tiled=True),
    )
    paired = jnp.stack([routed_keys[0], routed_values[0]]).reshape(
        2, groups * key_count, kv_own, HEAD_DIM
    )
    query_heads = query_rows.reshape(tokens, kv_own, per_kv, HEAD_DIM)
    group_rows = groups * key_count

    def locate(gathered):
        source_blk = gathered // group_rows
        within = gathered % group_rows
        source_grp = within // key_count
        slot_row = within % key_count
        return ((source_grp * blocks + source_blk) * key_count + slot_row).astype(jnp.int32)

    state = fold_keys(
        empty_state(kv_own, per_kv, tokens),
        lax.all_gather(paired, "blk", axis=1, tiled=True),
        query_heads,
        query_pos,
        table,
        locate,
        span_len,
        512,
    )
    mark, total, weighted = state
    mixed = weighted / total[..., None]
    mixed = jnp.transpose(mixed, (2, 0, 1, 3)).reshape(tokens, own_heads * HEAD_DIM)
    return mixed.astype(jnp.bfloat16)


def solution(mesh):
    in_specs = (P("blk", "grp"), P(("grp", "blk"), None), P(("grp", "blk"), None), P("blk"))
    out_specs = P("blk", "grp")
    return jax.shard_map(body, mesh=mesh, in_specs=in_specs, out_specs=out_specs, check_vma=False)
```
